256 devices in a mesh: row: 16 (over z, x_lo), col: 8 (over y, x_hi), depth: 2 (over core).
Axes of the slice: x: 4 (x_hi: 2, x_lo: 2; x = x_hi * 2 + x_lo), y: 4, z: 8, core: 2. Of those that a mesh axis runs over, the one named last changes fastest.
Arguments:
- matrix: float32 [2, 16, 512, 4, 8, 512], P(None, 'row', None, None, 'col'), may hold values from 0 to 5
Outputs:
- factored: float32 [2, 16, 512, 4, 8, 512], P(None, 'row', 'depth', None, 'col')
The draws below stay inside these ranges and needn't reach their ends.
All inputs are finite; a program needn't handle non-finite values.
Results may differ from the reference program's by a relative error of at most 0.00021.
Values sent between devices are 32-bit elements; how exact they have to be, the bound alone decides.
A program may use at most 128 MiB of HBM per device.

```python
import jax
import jax.numpy as jnp
from jax import lax

TILE = 512
NT = 32
STEPS = 2
TPR = 2
TPC = 4
N_ROW = 16
N_COL = 8


def draw_matrix(key, part):
    matrix_order = NT * TILE
    key_points, key_scale, key_lift = jax.random.split(jax.random.fold_in(key, 11), 3)
    points = jax.random.uniform(key_points, (matrix_order, 3), jnp.float32)
    length_scale = 2.0 / matrix_order ** (1.0 / 3.0)
    scales = jax.random.uniform(key_scale, (matrix_order,), jnp.float32, 0.7, 1.4)
    nugget = jax.random.uniform(key_lift, (matrix_order,), jnp.float32, 0.5, 1.0)
    distance = jnp.zeros((matrix_order, matrix_order), jnp.float32)
    for component in range(3):
        offset = points[:, component][:, None] - points[:, component][None, :]
        distance = distance + offset * offset
    kernel = scales[:, None] * scales[None, :] * jnp.exp(distance * (-0.5 / (length_scale * length_scale)))
    full_matrix = kernel + jnp.diag(nugget)
    return full_matrix.reshape(TPR, N_ROW, TILE, TPC, N_COL, TILE)


def setup_inputs(seed: int = 0) -> dict:
    streams_of = jax.random.split(jax.random.key(seed), 2)
    return {
        "matrix": draw_matrix(jax.random.fold_in(streams_of[1], 71), 0),
    }


def factor_diag(diag):
    diag_factor = jnp.linalg.cholesky(diag)
    inverse_factor = jax.scipy.linalg.solve_triangular(diag_factor, jnp.eye(diag.shape[0], dtype=jnp.float32), lower=True)
    return (diag_factor, inverse_factor)

def reference(matrix):
    matrix_order = NT * TILE
    current = matrix.reshape(matrix_order, matrix_order)
    lower = jnp.zeros((matrix_order, STEPS * TILE), jnp.float32)
    for section in range(STEPS):
        start = section * TILE
        finish = start + TILE
        diag_factor, inverse_factor = factor_diag(current[start:finish, start:finish])
        panel = jnp.dot(current[finish:, start:finish].astype(jnp.float32), inverse_factor.T.astype(jnp.float32), precision=lax.Precision.HIGHEST, preferred_element_type=jnp.float32)
        lower = lower.at[start:finish, start:finish].set(diag_factor)
        lower = lower.at[finish:, start:finish].set(panel)
        update = jnp.dot(panel.astype(jnp.float32), panel.T.astype(jnp.float32), precision=lax.Precision.HIGHEST, preferred_element_type=jnp.float32)
        current = current.at[finish:, finish:].add(-update)
    edge = STEPS * TILE
    result = jnp.zeros((matrix_order, matrix_order), jnp.float32)
    result = result.at[:, :edge].set(lower)
    result = result.at[edge:, edge:].set(current[edge:, edge:])
    return result.reshape(TPR, N_ROW, TILE, TPC, N_COL, TILE)
```

```python
import functools

import jax
import jax.numpy as jnp
from jax import lax
from jax.experimental import pallas as pl
from jax.experimental.pallas import tpu as pltpu
from jax.sharding import PartitionSpec as P

T = 512
B = 128
NB = 2 * T // B
RN = 32
RR = T // RN
CR = 64
HI = lax.Precision.HIGHEST
MESH = pl.DeviceIdType.MESH
F32 = jnp.float32
BF16 = jnp.bfloat16


def mm(a, b, dims=((1,), (0,)), precision=None):
    return lax.dot_general(a, b, (dims, ((), ())), precision=precision, preferred_element_type=F32)


def split(x):
    h = x.astype(BF16)
    return h, (x - h.astype(F32)).astype(BF16)


def mm3(a, b, dims=((1,), (0,))):
    return mm(a[0], b[0], dims) + (mm(a[0], b[1], dims) + mm(a[1], b[0], dims))


def base(a, w):
    out = []
    sub = lax.broadcasted_iota(jnp.int32, (8, B), 0)
    lane = lambda x, k: jnp.broadcast_to(x[:, k : k + 1], (8, B))
    row = lambda x, m: jnp.broadcast_to(x[m : m + 1, :], (8, B))
    for g in range(16):
        cg = [lane(a[g], 8 * g + n) for n in range(8)]
        e = [[row(cg[n], m) if n >= m else None for n in range(8)] for m in range(8)]
        ar = [row(a[g], m) for m in range(8)]
        wr = [row(w[g], m) for m in range(8)]
        rs = [None] * 8
        u = [[None] * 8 for _ in range(8)]
        for m in range(8):
            rs[m] = lax.rsqrt(e[m][m])
            for n in range(m + 1, 8):
                u[m][n] = e[m][n] * rs[m]
            ar[m] = ar[m] * rs[m]
            wr[m] = wr[m] * rs[m]
            for m2 in range(m + 1, 8):
                for n in range(m2, 8):
                    e[m2][n] = e[m2][n] - u[m][m2] * u[m][n]
                ar[m2] = ar[m2] - u[m][m2] * ar[m]
                wr[m2] = wr[m2] - u[m][m2] * wr[m]
        o = wr[0]
        for m in range(1, 8):
            o = jnp.where(sub == m, wr[m], o)
        out.append(o)
        for h in range(g + 1, 16):
            c = [lane(a[h], 8 * g + n) for n in range(8)]
            for m in range(8):
                f = c[m] * rs[m]
                for n in range(m + 1, 8):
                    c[n] = c[n] - f * u[m][n]
                a[h] = a[h] - f * ar[m]
                w[h] = w[h] - f * wr[m]
    return out


def kernel(
    x, out, rbuf, cbuf, fbuf, dbuf, abuf, vh, vl, lh, ll, wbuf, sbuf,
    r_rec, c_rec, f_rec, d_rec, rz_s, rx_s, rs_s, cy_s, cx_s, cs_s, f_s, d_s, loc,
):
    p, q, d = lax.axis_index("row"), lax.axis_index("col"), lax.axis_index("depth")
    z, xl = p // 2, p % 2
    y, xh = q // 2, q % 2
    xx = xh * 2 + xl
    dev = lambda zz, xli, yy, xhi, dd: (zz * 2 + xli, yy * 2 + xhi, dd)
    sib = dev(z, xl, y, xh, 1 - d)
    both = jnp.logical_and

    def remote(src, dst, ssem, rsem, to):
        return pltpu.make_async_remote_copy(
            src_ref=src, dst_ref=dst, send_sem=ssem, recv_sem=rsem, device_id=to, device_id_type=MESH
        )

    def arrived(dst, rsem):
        pltpu.make_async_copy(dst, dst, rsem).wait()

    def when_start(cond, copy, op):
        @pl.when(cond)
        def _():
            c = copy()
            c.start() if op else c.wait_send()

    rpiece = lambda k, n: rbuf.at[pl.ds(pl.multiple_of(k * T + n * RR, 8), RR), :]
    xr = lambda n: x.at[pl.ds(pl.multiple_of(n * RR, 8), RR), :]

    def cpiece(k, h, s, r):
        return cbuf.at[
            pl.ds(pl.multiple_of(h * T + s * 256 + r * CR, 8), CR), pl.ds(pl.multiple_of(k * T, B), T)
        ]

    xc = lambda h, s, r: x.at[pl.ds(pl.multiple_of(s * T + h * 256 + r * CR, 8), CR), pl.ds(0, T)]
    fpiece = lambda b, c: fbuf.at[pl.ds(pl.multiple_of(b * B, B), B), pl.ds(pl.multiple_of(c * B, B), B)]

    def r_own(n, src, op):
        up = n % 2 == 0
        nxt = jnp.where(up, (z + 1) % 8, (z + 7) % 8)
        more = jnp.where(up, z != 7, z != 1)
        when_start(
            more, lambda: remote(src, rpiece(xl, n), rz_s.at[n], r_rec.at[xl, n], dev(nxt, xl, y, xh, 0)), op
        )
        when_start(
            z >= 0, lambda: remote(src, rpiece(xl, n), rx_s.at[n], r_rec.at[xl, n], dev(z, 1 - xl, y, xh, 0)), op
        )

    def r_sib(k, n, op):
        when_start(
            z >= 0, lambda: remote(rpiece(k, n), rpiece(k, n), rs_s.at[k, n], r_rec.at[k, n], sib), op
        )

    def c_next(k, h, s, r, src, op):
        i = (k * 2 + s) * 4 + r
        nxt = jnp.where(h == 0, (y + 1) % 4, (y + 3) % 4)
        more = jnp.where(h == 0, y != 3, y != 1)
        when_start(
            more, lambda: remote(src, cpiece(k, h, s, r), cy_s.at[h, i], c_rec.at[h, i], dev(z, xl, nxt, xh, 0)), op
        )

    def c_cross(k, h, s, r, src, op):
        i = (k * 2 + s) * 4 + r
        when_start(
            z >= 0,
            lambda: remote(src, cpiece(k, h, s, r), cx_s.at[h, i], c_rec.at[h, i], dev(z, xl, y, 1 - xh, 0)), op,
        )

    def c_sib(k, h, s, r, op):
        i = (k * 2 + s) * 4 + r
        when_start(
            h == 1,
            lambda: remote(cpiece(k, h, s, r), cpiece(k, h, s, r), cs_s.at[i], c_rec.at[h, i], sib), op,
        )

    def f_send(b, c, op):
        v = fpiece(b, c)
        i = b * NB + c
        go = lambda cond, slot, to: when_start(
            cond, lambda: remote(v, v, f_s.at[slot, i], f_rec.at[i], to), op
        )
        root_line = both(z == 0, y == 0)
        go(both(root_line, xx == 0), 0, dev(z, 1, y, 0, 1))
        go(both(root_line, xx == 0), 1, dev(z, 1, y, 1, 1))
        go(both(root_line, xx == 1), 1, dev(z, 0, y, 1, 1))
        plane = y == 0
        go(both(plane, z <= 3), 2, dev((z + 1) % 8, xl, y, xh, 1))
        go(both(plane, (z == 0) | (z >= 6)), 3, dev((z + 7) % 8, xl, y, xh, 1))
        go((y == 0) | (y == 1), 4, dev(z, xl, (y + 1) % 4, xh, 1))
        go(y == 0, 5, dev(z, xl, (y + 3) % 4, xh, 1))
        go(z >= 0, 6, sib)

    def loop(n, f):
        lax.fori_loop(0, n, lambda i, s: (f(i), s)[1], 0)

    is_root = both(both(p == 0, q == 0), d == 1)
    src_r = z == 0
    src_c = y == 0

    own = [
        pltpu.make_async_copy(
            x.at[pl.ds(pl.multiple_of(s * T + d * 256, 8), 256), :], abuf.at[pl.ds(s * 256, 256), :], loc.at[s]
        )
        for s in range(2)
    ]
    for c in own:
        c.start()
    r_loc = pltpu.make_async_copy(
        x.at[pl.ds(0, T), :], rbuf.at[pl.ds(pl.multiple_of(xl * T, 8), T), :], loc.at[2]
    )
    c_loc = [
        pltpu.make_async_copy(
            x.at[pl.ds(pl.multiple_of(s * T + d * 256, 8), 256), pl.ds(0, T)],
            cbuf.at[pl.ds(pl.multiple_of(d * T + s * 256, 8), 256), pl.ds(pl.multiple_of(xh * T, B), T)],
            loc.at[3 + s],
        )
        for s in range(2)
    ]
    d_loc = pltpu.make_async_copy(x.at[pl.ds(0, T), pl.ds(0, T)], dbuf.at[pl.ds(0, T), pl.ds(0, T)], loc.at[5])

    @pl.when(src_r)
    def _():
        r_loc.start()

    @pl.when(src_c)
    def _():
        for c in c_loc:
            c.start()

    def d_copies(op):
        for i in range(4):
            when_start(
                both(both(p == 0, q == 1), d == 1),
                lambda: remote(
                    x.at[pl.ds(i * B, B), pl.ds(0, T)], dbuf.at[pl.ds(i * B, B), pl.ds(T, T)],
                    d_s.at[i], d_rec.at[i], (0, 0, 1),
                ),
                op,
            )
        when_start(
            both(both(p == 1, q == 1), d == 1),
            lambda: remote(
                x.at[pl.ds(0, T), pl.ds(0, T)], dbuf.at[pl.ds(T, T), pl.ds(T, T)], d_s.at[4], d_rec.at[4], (0, 0, 1)
            ),
            op,
        )

    d_copies(True)

    def source_copies(op):
        @pl.when(both(src_r, d == 0))
        def _():
            loop(RN, lambda n: r_own(n, xr(n), op))

        @pl.when(both(src_c, d == 0))
        def _():
            def one(i):
                for h in range(2):
                    c_next(xh, h, i // 4, i % 4, xc(h, i // 4, i % 4), op)
                    c_cross(xh, h, i // 4, i % 4, xc(h, i // 4, i % 4), op)

            loop(8, one)

    def forward(op):
        def step(t):
            for up in range(2):
                hops = z if up == 0 else 8 - z
                e = t - 2 * hops
                n = 2 * e + up

                @pl.when(both(both(e >= 0, e < RN // 2), z != 0))
                def _():
                    if op:
                        arrived(rpiece(xl, n), r_rec.at[xl, n])
                    r_own(n, rpiece(xl, n), op)
                    r_sib(xl, n, op)

                e2 = t - 2 * jnp.where(z == 0, 0, hops) - 2
                n2 = 2 * e2 + up

                @pl.when(both(e2 >= 0, e2 < RN // 2))
                def _():
                    if op:
                        arrived(rpiece(1 - xl, n2), r_rec.at[1 - xl, n2])
                    r_sib(1 - xl, n2, op)

            for h in range(2):
                hops = y if h == 0 else (4 - y) % 4
                e = t - 2 * hops - 2
                c = e % 16
                first = c < 8
                k = jnp.where(first, xh, 1 - xh)
                s, r = (c % 8) // 4, c % 4

                @pl.when(both(both(e >= 0, e < 16), (y != 0) | (k != xh)))
                def _():
                    i = (k * 2 + s) * 4 + r
                    if op:
                        arrived(cpiece(k, h, s, r), c_rec.at[h, i])
                    c_next(k, h, s, r, cpiece(k, h, s, r), op)
                    c_sib(k, h, s, r, op)

        loop(16 + 14 + 2, step)

    source_copies(True)

    def f_all(f):
        def rows(b):
            lax.fori_loop(b, NB, lambda c, s: (f(b, c), s)[1], 0)

        loop(NB, rows)

    @pl.when(is_root)
    def _():
        d_loc.start()
        d_loc.wait()
        lanes = lax.broadcasted_iota(jnp.int32, (8, B), 1)
        subs = lax.broadcasted_iota(jnp.int32, (8, B), 0)

        def factor(b):
            for v in range(NB):

                @pl.when(b == v)
                def _():
                    if v == 4:
                        arrived(dbuf.at[pl.ds(T, T), pl.ds(T, T)], d_rec.at[4])
                    s = dbuf[v * B : (v + 1) * B, v * B : (v + 1) * B]
                    if v:
                        u = fbuf[: v * B, v * B : (v + 1) * B]
                        s = s - mm(u, u, ((0,), (0,)), HI)
                    sbuf[:, :B] = s

            a = [sbuf[8 * h : 8 * h + 8, 0:B] for h in range(16)]
            w = [jnp.where(lanes == subs + 8 * h, 1.0, 0.0) for h in range(16)]
            o = base(a, w)
            for v in range(NB):

                @pl.when(b == v)
                def _():
                    for h in range(16):
                        fbuf[v * B + 8 * h : v * B + 8 * h + 8, v * B : (v + 1) * B] = o[h]
                    if v < 4:
                        arrived(dbuf.at[pl.ds(v * B, B), pl.ds(T, T)], d_rec.at[v])
                    if v < NB - 1:
                        s = dbuf[v * B : (v + 1) * B, (v + 1) * B :]
                        if v:
                            s = s - mm(
                                fbuf[: v * B, v * B : (v + 1) * B], fbuf[: v * B, (v + 1) * B :], ((0,), (0,)), HI
                            )
                        wv = fbuf[v * B : (v + 1) * B, v * B : (v + 1) * B]
                        fbuf[v * B : (v + 1) * B, (v + 1) * B :] = mm(wv, s, precision=HI)

            lax.fori_loop(b, NB, lambda c, s: (f_send(b, c, True), s)[1], 0)

        loop(NB, factor)

    @pl.when(both(d == 1, jnp.logical_not(is_root)))
    def _():
        def pass_on(b, c):
            arrived(fpiece(b, c), f_rec.at[b * NB + c])
            f_send(b, c, True)

        f_all(pass_on)

    @pl.when(d == 0)
    def _():
        forward(True)
        f_all(lambda b, c: arrived(fpiece(b, c), f_rec.at[b * NB + c]))

    @pl.when(d == 1)
    def _():
        def one(n):
            @pl.when(z != 0)
            def _():
                arrived(rpiece(xl, n), r_rec.at[xl, n])

            arrived(rpiece(1 - xl, n), r_rec.at[1 - xl, n])

        loop(RN, one)

        def two(i):
            k, s, r = i // 8, (i % 8) // 4, i % 4

            @pl.when((y != 0) | (k != xh))
            def _():
                arrived(cpiece(k, 1, s, r), c_rec.at[1, i])

        loop(16, two)

    @pl.when(src_r)
    def _():
        r_loc.wait()

    @pl.when(src_c)
    def _():
        for c in c_loc:
            c.wait()

    G = 256
    crow = pl.ds(pl.multiple_of(d * T, 8), T)
    for g in range(2 * T // G):
        at = g * G
        w1 = fbuf[at : at + B, at : at + B]
        w2 = fbuf[at + B : at + G, at + B : at + G]
        u12 = fbuf[at : at + B, at + B : at + G]
        w21 = -mm(w2, mm(u12, w1, ((0,), (0,)), HI), precision=HI)
        wbuf[:B, :B] = w1
        wbuf[:B, B:] = jnp.zeros((B, B), F32)
        wbuf[B:, :B] = w21
        wbuf[B:, B:] = w2
        w = split(wbuf[...])
        wt = split(wbuf[...].T)
        if g:
            uf = fbuf[:at, at : at + G]
            u = split(uf)
            ut = split(uf.T)
        acc = cbuf[crow, at : at + G]
        if g:
            acc = acc - mm3((lh[:, :at], ll[:, :at]), u)
        a, b = split(mm3(split(acc), wt))
        lh[:, at : at + G] = a
        ll[:, at : at + G] = b

        def columns(n):
            cols = pl.ds(pl.multiple_of(n * T, B), T)
            acc = rbuf[at : at + G, cols]
            if g:
                acc = acc - mm3(ut, (vh[:at, cols], vl[:at, cols]))
            a, b = split(mm3(w, split(acc)))
            vh[at : at + G, cols] = a
            vl[at : at + G, cols] = b

        loop(4, columns)

    for c in own:
        c.wait()

    def store(n):
        return pltpu.make_async_copy(
            abuf.at[:, pl.ds(pl.multiple_of(n * T, B), T)],
            out.at[:, pl.ds(pl.multiple_of(n * T, B), T)],
            loc.at[6 + n],
        )

    def update(n):
        cols = pl.ds(pl.multiple_of(n * T, B), T)
        for s in range(2):
            rows = slice(s * 256, s * 256 + 256)
            res = abuf[rows, cols] - mm3((lh[rows, :], ll[rows, :]), (vh[:, cols], vl[:, cols]))
            if s == 0:
                res = jnp.where(p < 2, 0.0, res)
            abuf[rows, cols] = res

        @pl.when(both(n == 0, q < 2))
        def _():
            pick = pl.ds(pl.multiple_of(q * T, B), T)
            for s in range(2):
                rows = slice(s * 256, s * 256 + 256)
                res = lh[rows, pick].astype(F32) + ll[rows, pick].astype(F32)
                if s == 0:
                    i = lax.broadcasted_iota(jnp.int32, (256, T), 0) + d * 256
                    j = lax.broadcasted_iota(jnp.int32, (256, T), 1)
                    res = jnp.where((p > q) | ((p == q) & (i >= j)), res, 0.0)
                abuf[rows, 0:T] = res

        store(n).start()

    loop(4, update)
    loop(4, lambda n: store(n).wait())

    d_copies(False)
    source_copies(False)

    @pl.when(d == 0)
    def _():
        forward(False)

    @pl.when(d == 1)
    def _():
        f_all(lambda b, c: f_send(b, c, False))


def call(x):
    dma = pltpu.SemaphoreType.DMA
    return pl.pallas_call(
        kernel,
        out_shape=jax.ShapeDtypeStruct((T, 4 * T), F32),
        in_specs=[pl.BlockSpec(memory_space=pl.ANY)],
        out_specs=pl.BlockSpec(memory_space=pl.ANY),
        scratch_shapes=[
            pltpu.VMEM((2 * T, 4 * T), F32),
            pltpu.VMEM((2 * T, 2 * T), F32),
            pltpu.VMEM((2 * T, 2 * T), F32),
            pltpu.VMEM((2 * T, 2 * T), F32),
            pltpu.VMEM((T, 4 * T), F32),
            pltpu.VMEM((2 * T, 4 * T), BF16),
            pltpu.VMEM((2 * T, 4 * T), BF16),
            pltpu.VMEM((T, 2 * T), BF16),
            pltpu.VMEM((T, 2 * T), BF16),
            pltpu.VMEM((256, 256), F32),
            pltpu.VMEM((B, B), F32),
            dma((2, RN)),
            dma((2, 16)),
            dma((NB * NB,)),
            dma((5,)),
            dma((RN,)),
            dma((RN,)),
            dma((2, RN)),
            dma((2, 16)),
            dma((2, 16)),
            dma((16,)),
            dma((7, NB * NB)),
            dma((5,)),
            dma((10,)),
        ],
        compiler_params=pltpu.CompilerParams(has_side_effects=True, vmem_limit_bytes=56 * 1024 * 1024),
        name="panels",
    )(x)


def body(matrix):
    return call(matrix.reshape(2 * T, 4 * T)).reshape(2, 1, T // 2, 4, 1, T)


def solution(mesh):
    return jax.shard_map(
        body,
        mesh=mesh,
        in_specs=(P(None, "row", None, None, "col", None),),
        out_specs=P(None, "row", "depth", None, "col", None),
        check_vma=False,
    )
```

```python
import functools

import jax
import jax.numpy as jnp
from jax import lax
from jax.experimental import pallas as pl
from jax.experimental.pallas import tpu as pltpu
from jax.sharding import PartitionSpec as P

T = 512
B = 128
NB = 2 * T // B
RN = 32
RR = T // RN
CR = 64
L16 = 4 * T // B
SCHED = (8, 8, 8, 8)
HI = lax.Precision.HIGHEST
MESH = pl.DeviceIdType.MESH
F32 = jnp.float32
BF16 = jnp.bfloat16


def mm(a, b, dims=((1,), (0,)), precision=None):
    return lax.dot_general(a, b, (dims, ((), ())), precision=precision, preferred_element_type=F32)


def split(x):
    h = x.astype(BF16)
    return h, (x - h.astype(F32)).astype(BF16)


def mm3(a, b, dims=((1,), (0,))):
    return mm(a[0], b[0], dims) + (mm(a[0], b[1], dims) + mm(a[1], b[0], dims))


def base(a, w):
    out = []
    sub = lax.broadcasted_iota(jnp.int32, (8, B), 0)
    lane = lambda x, k: jnp.broadcast_to(x[:, k : k + 1], (8, B))
    row = lambda x, m: jnp.broadcast_to(x[m : m + 1, :], (8, B))
    for g in range(16):
        cg = [lane(a[g], 8 * g + n) for n in range(8)]
        e = [[row(cg[n], m) if n >= m else None for n in range(8)] for m in range(8)]
        ar = [row(a[g], m) for m in range(8)]
        wr = [row(w[g], m) for m in range(8)]
        rs = [None] * 8
        u = [[None] * 8 for _ in range(8)]
        for m in range(8):
            rs[m] = lax.rsqrt(e[m][m])
            for n in range(m + 1, 8):
                u[m][n] = e[m][n] * rs[m]
            ar[m] = ar[m] * rs[m]
            wr[m] = wr[m] * rs[m]
            for m2 in range(m + 1, 8):
                for n in range(m2, 8):
                    e[m2][n] = e[m2][n] - u[m][m2] * u[m][n]
                ar[m2] = ar[m2] - u[m][m2] * ar[m]
                wr[m2] = wr[m2] - u[m][m2] * wr[m]
        o = wr[0]
        for m in range(1, 8):
            o = jnp.where(sub == m, wr[m], o)
        out.append(o)
        for h in range(g + 1, 16):
            c = [lane(a[h], 8 * g + n) for n in range(8)]
            for m in range(8):
                f = c[m] * rs[m]
                for n in range(m + 1, 8):
                    c[n] = c[n] - f * u[m][n]
                a[h] = a[h] - f * ar[m]
                w[h] = w[h] - f * wr[m]
    return out


def kernel(
    x, xq, abuf, rbuf, cbuf, fbuf, dbuf, vh, vl, lh, ll, wbuf, sbuf, part,
    r_rec, c_rec, f_rec, d_rec, rz_s, rx_s, rs_s, cy_s, cx_s, cs_s, f_s, d_s, loc,
):
    p, q, d = lax.axis_index("row"), lax.axis_index("col"), lax.axis_index("depth")
    z, xl = p // 2, p % 2
    y, xh = q // 2, q % 2
    xx = xh * 2 + xl
    dev = lambda zz, xli, yy, xhi, dd: (zz * 2 + xli, yy * 2 + xhi, dd)
    sib = dev(z, xl, y, xh, 1 - d)
    both = jnp.logical_and

    def remote(src, dst, ssem, rsem, to):
        return pltpu.make_async_remote_copy(
            src_ref=src, dst_ref=dst, send_sem=ssem, recv_sem=rsem, device_id=to, device_id_type=MESH
        )

    def arrived(dst, rsem):
        pltpu.make_async_copy(dst, dst, rsem).wait()

    def when_start(cond, copy, op):
        @pl.when(cond)
        def _():
            c = copy()
            c.start() if op else c.wait_send()

    is_root = both(both(p == 0, q == 0), d == 1)
    src_r = z == 0
    src_c = y == 0

    own = [
        pltpu.make_async_copy(
            x.at[pl.ds(pl.multiple_of((s * T + d * 256) * L16, 8), 256 * L16), :],
            abuf.at[pl.ds(s * 256 * L16, 256 * L16), :],
            loc.at[s],
        )
        for s in range(2)
    ]
    for c in own:
        c.start()
    r_loc = pltpu.make_async_copy(
        x.at[pl.ds(0, T * L16), :], rbuf.at[pl.ds(pl.multiple_of(xl * T * L16, 8), T * L16), :], loc.at[2]
    )
    c_loc = [
        pltpu.make_async_copy(
            xq.at[pl.ds(s * T + d * 256, 256), 0], cbuf.at[xh, pl.ds(d * T + s * 256, 256)], loc.at[3 + s]
        )
        for s in range(2)
    ]
    d_loc = pltpu.make_async_copy(xq.at[pl.ds(0, T), 0], dbuf.at[0, pl.ds(0, T)], loc.at[5])

    @pl.when(src_r)
    def _():
        r_loc.start()

    @pl.when(src_c)
    def _():
        for c in c_loc:
            c.start()

    @pl.when(is_root)
    def _():
        d_loc.start()

    near = [
        sib,
        dev((z + 1) % 8, xl, y, xh, d), dev((z + 7) % 8, xl, y, xh, d),
        dev(z, xl, (y + 1) % 4, xh, d), dev(z, xl, (y + 3) % 4, xh, d),
        dev(z, 1 - xl, y, xh, d), dev(z, xl, y, 1 - xh, d), dev(z, 1 - xl, y, 1 - xh, d),
    ]
    barrier = pltpu.get_barrier_semaphore()
    for to in near:
        pl.semaphore_signal(barrier, inc=1, device_id=to, device_id_type=MESH)
    pl.semaphore_wait(barrier, len(near))

    rpiece = lambda k, n: rbuf.at[pl.ds(pl.multiple_of((k * T + n * RR) * L16, 8), RR * L16), :]
    xr = lambda n: x.at[pl.ds(pl.multiple_of(n * RR * L16, 8), RR * L16), :]

    def cpiece(k, h, s, r):
        return cbuf.at[k, pl.ds(h * T + s * 256 + r * CR, CR)]

    xc = lambda h, s, r: xq.at[pl.ds(s * T + h * 256 + r * CR, CR), 0]
    fpiece = lambda b, c: fbuf.at[pl.ds(pl.multiple_of(b * B, B), B), pl.ds(pl.multiple_of(c * B, B), B)]

    def r_own(n, src, op):
        up = n % 2 == 0
        nxt = jnp.where(up, (z + 1) % 8, (z + 7) % 8)
        more = jnp.where(up, z != 7, z != 1)
        when_start(
            more, lambda: remote(src, rpiece(xl, n), rz_s.at[n], r_rec.at[xl, n], dev(nxt, xl, y, xh, 0)), op
        )
        when_start(
            z >= 0, lambda: remote(src, rpiece(xl, n), rx_s.at[n], r_rec.at[xl, n], dev(z, 1 - xl, y, xh, 0)), op
        )

    def r_sib(k, n, op):
        when_start(
            z >= 0, lambda: remote(rpiece(k, n), rpiece(k, n), rs_s.at[k, n], r_rec.at[k, n], sib), op
        )

    def c_next(k, h, s, r, src, more, op):
        i = (k * 2 + s) * 4 + r
        nxt = jnp.where(h == 0, (y + 1) % 4, (y + 3) % 4)
        when_start(
            more, lambda: remote(src, cpiece(k, h, s, r), cy_s.at[h, i], c_rec.at[h, i], dev(z, xl, nxt, xh, 0)), op
        )

    def c_cross(k, h, s, r, src, op):
        i = (k * 2 + s) * 4 + r
        when_start(
            y == (r + 2 * h) % 4,
            lambda: remote(src, cpiece(k, h, s, r), cx_s.at[h, i], c_rec.at[h, i], dev(z, xl, y, 1 - xh, 0)), op,
        )

    def c_sib(k, h, s, r, op):
        i = (k * 2 + s) * 4 + r
        when_start(
            h == 1,
            lambda: remote(cpiece(k, h, s, r), cpiece(k, h, s, r), cs_s.at[i], c_rec.at[h, i], sib), op,
        )

    def f_send(b, c, op):
        v = fpiece(b, c)
        i = b * NB + c
        go = lambda cond, slot, to: when_start(
            cond, lambda: remote(v, v, f_s.at[slot, i], f_rec.at[i], to), op
        )
        root_line = both(z == 0, y == 0)
        go(both(root_line, xx == 0), 0, dev(z, 1, y, 0, 1))
        go(both(root_line, xx == 0), 1, dev(z, 1, y, 1, 1))
        go(both(root_line, xx == 1), 1, dev(z, 0, y, 1, 1))
        plane = y == 0
        go(both(plane, z <= 3), 2, dev((z + 1) % 8, xl, y, xh, 1))
        go(both(plane, (z == 0) | (z >= 6)), 3, dev((z + 7) % 8, xl, y, xh, 1))
        go((y == 0) | (y == 1), 4, dev(z, xl, (y + 1) % 4, xh, 1))
        go(y == 0, 5, dev(z, xl, (y + 3) % 4, xh, 1))
        go(z >= 0, 6, sib)

    def loop(n, f):
        lax.fori_loop(0, n, lambda i, s: (f(i), s)[1], 0)

    def d_copies(op):
        for i in range(4):
            when_start(
                both(both(p == 0, q == 1), d == 1),
                lambda: remote(
                    xq.at[pl.ds(i * B, B), 0], dbuf.at[1, pl.ds(i * B, B)], d_s.at[i], d_rec.at[i], (0, 0, 1)
                ),
                op,
            )
        when_start(
            both(both(p == 1, q == 1), d == 1),
            lambda: remote(
                xq.at[pl.ds(0, T), 0], dbuf.at[1, pl.ds(T, T)], d_s.at[4], d_rec.at[4], (0, 0, 1)
            ),
            op,
        )

    d_copies(True)

    def source_copies(op):
        @pl.when(both(src_c, d == 0))
        def _():
            def one(i):
                s, r = i // 4, i % 4
                for h in range(2):
                    c_next(xh, h, s, r, xc(h, s, r), z >= 0, op)
                    c_cross(xh, h, s, r, xc(h, s, r), op)

            loop(8, one)

        @pl.when(both(src_r, d == 0))
        def _():
            loop(RN, lambda n: r_own(n, xr(n), op))

    def forward(op):
        def own_line(t):
            for up in range(2):
                hops = z if up == 0 else 8 - z
                e = t - 3 * hops
                n = 2 * e + up

                @pl.when(both(both(e >= 0, e < RN // 2), z != 0))
                def _():
                    if op:
                        arrived(rpiece(xl, n), r_rec.at[xl, n])
                    r_own(n, rpiece(xl, n), op)
                    r_sib(xl, n, op)

            for h in range(2):
                hops = y if h == 0 else (4 - y) % 4
                e = t - 3 * hops
                on = z >= 0

                @pl.when(both(both(e >= 0, e < 8), both(y != 0, on)))
                def _():
                    s, r = e // 4, e % 4
                    if op:
                        arrived(cpiece(xh, h, s, r), c_rec.at[h, (xh * 2 + s) * 4 + r])
                    c_next(xh, h, s, r, cpiece(xh, h, s, r), hops != 3, op)
                    c_cross(xh, h, s, r, cpiece(xh, h, s, r), op)
                    c_sib(xh, h, s, r, op)

        loop(max(RN // 2 + 7 * 3, 8 * 1 + 3 * 3), own_line)

        def other_line(j):
            for h in range(2):
                r = (y + j + 2 * h) % 4 if h else (y - j + 4) % 4
                for s in range(2):
                    k = 1 - xh
                    if op:
                        arrived(cpiece(k, h, s, r), c_rec.at[h, (k * 2 + s) * 4 + r])
                    c_next(k, h, s, r, cpiece(k, h, s, r), j != 3, op)
                    c_sib(k, h, s, r, op)

        loop(4, other_line)

        def across(t):
            for up in range(2):
                hops = z if up == 0 else 8 - z
                e = t - 3 * jnp.where(z == 0, 0, hops)
                n = 2 * e + up

                @pl.when(both(e >= 0, e < RN // 2))
                def _():
                    if op:
                        arrived(rpiece(1 - xl, n), r_rec.at[1 - xl, n])
                    r_sib(1 - xl, n, op)

        loop(RN // 2 + 7 * 3, across)

    source_copies(True)

    @pl.when(is_root)
    def _():
        d_loc.wait()
        lanes = lax.broadcasted_iota(jnp.int32, (8, B), 1)
        subs = lax.broadcasted_iota(jnp.int32, (8, B), 0)

        def dblock(v, c):
            return dbuf[c // 4, v * B : (v + 1) * B, c % 4, :]

        def factor(b):
            for v in range(NB):

                @pl.when(b == v)
                def _():
                    if v == 4:
                        arrived(dbuf.at[1, pl.ds(T, T)], d_rec.at[4])
                    s = dblock(v, v)
                    if v:
                        u = fbuf[: v * B, v * B : (v + 1) * B]
                        s = s - mm(u, u, ((0,), (0,)), HI)
                    sbuf[:, :B] = s

            a = [sbuf[8 * h : 8 * h + 8, 0:B] for h in range(16)]
            w = [jnp.where(lanes == subs + 8 * h, 1.0, 0.0) for h in range(16)]
            o = base(a, w)
            for v in range(NB):

                @pl.when(b == v)
                def _():
                    for h in range(16):
                        fbuf[v * B + 8 * h : v * B + 8 * h + 8, v * B : (v + 1) * B] = o[h]
                    if v < 4:
                        arrived(dbuf.at[1, pl.ds(v * B, B)], d_rec.at[v])
                    if v < NB - 1:
                        s = jnp.concatenate([dblock(v, c) for c in range(v + 1, NB)], axis=1)
                        if v:
                            s = s - mm(
                                fbuf[: v * B, v * B : (v + 1) * B], fbuf[: v * B, (v + 1) * B :], ((0,), (0,)), HI
                            )
                        wv = fbuf[v * B : (v + 1) * B, v * B : (v + 1) * B]
                        fbuf[v * B : (v + 1) * B, (v + 1) * B :] = mm(wv, s, precision=HI)

            lax.fori_loop(b, NB, lambda c, s: (f_send(b, c, True), s)[1], 0)

        loop(NB, factor)

    @pl.when(d == 0)
    def _():
        forward(True)

    passes = both(d == 1, jnp.logical_not(is_root))

    def pass_on(b, c):
        arrived(fpiece(b, c), f_rec.at[b * NB + c])
        f_send(b, c, True)

    def take(b, c):
        arrived(fpiece(b, c), f_rec.at[b * NB + c])

    def f_rows(first, last, f):
        def rows(b, _):
            lax.fori_loop(b, NB, lambda c, s: (f(b, c), s)[1], 0)
            return 0

        lax.fori_loop(first, last, rows, 0)

    def panels_here(k, half):
        @pl.when(d == 1)
        def _():
            def one(i):
                n = half * (RN // 2) + i

                @pl.when((z != 0) | (k != xl))
                def _():
                    arrived(rpiece(k, n), r_rec.at[k, n])

            loop(RN // 2, one)

            def two(i):
                @pl.when((y != 0) | (k != xh))
                def _():
                    arrived(cpiece(k, 1, i // 4, i % 4), c_rec.at[1, k * 8 + i])

            if half == 0:
                loop(8, two)

        if half == 0:

            @pl.when(both(src_r, k == xl))
            def _():
                r_loc.wait()

            @pl.when(both(src_c, k == xh))
            def _():
                for c in c_loc:
                    c.wait()

    G = 256
    crow = pl.ds(d * T, T)

    def rload(at, n):
        return jnp.concatenate([rbuf[pl.ds(at * L16 + n * 4 + c, G, stride=L16), :] for c in range(4)], axis=1)

    def aload(s, n):
        return jnp.concatenate(
            [abuf[pl.ds(s * 256 * L16 + n * 4 + c, 256, stride=L16), :] for c in range(4)], axis=1
        )

    def astore(s, n, val):
        for c in range(4):
            abuf[pl.ds(s * 256 * L16 + n * 4 + c, 256, stride=L16), :] = val[:, c * B : (c + 1) * B]

    for g in range(2 * T // G):
        at = g * G
        if SCHED[g] > (SCHED[g - 1] if g else 0):

            @pl.when(passes)
            def _():
                f_rows(SCHED[g - 1] if g else 0, SCHED[g], pass_on)

        panels_here(g // 2, g % 2)
        if g == 0:
            for c in own:
                c.wait()
        c4 = (at % T) // B
        acc = jnp.concatenate([cbuf[g // 2, crow, c4 + c, :] for c in range(2)], axis=1)
        if g:
            uf = fbuf[:at, at : at + G]
            u = split(uf)
            ut = split(uf.T)
            acc = acc - mm3((lh[:, :at], ll[:, :at]), u)

            def before(n):
                cols = pl.ds(pl.multiple_of(n * T, B), T)
                part[:, cols] = rload(at, n) - mm3(ut, (vh[:at, cols], vl[:at, cols]))

            loop(4, before)
        wbuf[:, :G] = acc

        @pl.when(d == 0)
        def _():
            f_rows(2 * g, 2 * g + 2, take)

        w1 = fbuf[at : at + B, at : at + B]
        w2 = fbuf[at + B : at + G, at + B : at + G]
        u12 = fbuf[at : at + B, at + B : at + G]
        w21 = -mm(w2, mm(u12, w1, ((0,), (0,)), HI), precision=HI)
        w = jnp.concatenate(
            [jnp.concatenate([w1, jnp.zeros((B, B), F32)], axis=1), jnp.concatenate([w21, w2], axis=1)], axis=0
        )
        wt = split(w.T)
        w = split(w)
        a, b = split(mm3(split(wbuf[...]), wt))
        lh[:, at : at + G] = a
        ll[:, at : at + G] = b

        def columns(n):
            cols = pl.ds(pl.multiple_of(n * T, B), T)
            a, b = split(mm3(w, split(part[:, cols] if g else rload(at, n))))
            vh[at : at + G, cols] = a
            vl[at : at + G, cols] = b
            for s in range(2):
                rows = slice(s * 256, s * 256 + 256)
                res = aload(s, n) - mm3((lh[rows, at : at + G], ll[rows, at : at + G]), (a, b))
                if s == 0 and g == 3:
                    res = jnp.where(p < 2, 0.0, res)
                astore(s, n, res)

        loop(4, columns)

    @pl.when(q < 2)
    def _():
        pick = pl.ds(pl.multiple_of(q * T, B), T)
        for s in range(2):
            rows = slice(s * 256, s * 256 + 256)
            res = lh[rows, pick].astype(F32) + ll[rows, pick].astype(F32)
            if s == 0:
                i = lax.broadcasted_iota(jnp.int32, (256, T), 0) + d * 256
                j = lax.broadcasted_iota(jnp.int32, (256, T), 1)
                res = jnp.where((p > q) | ((p == q) & (i >= j)), res, 0.0)
            astore(s, 0, res)

    d_copies(False)
    source_copies(False)

    @pl.when(d == 0)
    def _():
        forward(False)

    @pl.when(d == 1)
    def _():
        f_rows(0, NB, lambda b, c: f_send(b, c, False))


def call(x, xq):
    dma = pltpu.SemaphoreType.DMA
    return pl.pallas_call(
        kernel,
        out_shape=pltpu.VMEM((T * L16, B), F32),
        in_specs=[pl.BlockSpec(memory_space=pltpu.HBM)] * 2,
        out_specs=pl.BlockSpec(memory_space=pltpu.VMEM),
        scratch_shapes=[
            pltpu.VMEM((2 * T * L16, B), F32),
            pltpu.VMEM((2, 2 * T, 4, B), F32),
            pltpu.VMEM((2 * T, 2 * T), F32),
            pltpu.VMEM((2, 2 * T, 4, B), F32),
            pltpu.VMEM((2 * T, 4 * T), BF16),
            pltpu.VMEM((2 * T, 4 * T), BF16),
            pltpu.VMEM((T, 2 * T), BF16),
            pltpu.VMEM((T, 2 * T), BF16),
            pltpu.VMEM((T, 256), F32),
            pltpu.VMEM((B, B), F32),
            pltpu.VMEM((256, 4 * T), F32),
            dma((2, RN)),
            dma((2, 16)),
            dma((NB * NB,)),
            dma((5,)),
            dma((RN,)),
            dma((RN,)),
            dma((2, RN)),
            dma((2, 16)),
            dma((2, 16)),
            dma((16,)),
            dma((7, NB * NB)),
            dma((5,)),
            dma((7,)),
        ],
        compiler_params=pltpu.CompilerParams(collective_id=0, has_side_effects=True, vmem_limit_bytes=56 * 1024 * 1024),
        name="panels",
    )(x, xq)


def body(matrix):
    out = call(matrix.reshape(2 * T * L16, B), matrix.reshape(2 * T, 4, 4, B))
    return out.reshape(2, 1, T // 2, 4, 1, T)


def solution(mesh):
    return jax.shard_map(
        body,
        mesh=mesh,
        in_specs=(P(None, "row", None, None, "col", None),),
        out_specs=P(None, "row", "depth", None, "col", None),
        check_vma=False,
    )
```

```python
import functools

import jax
import jax.numpy as jnp
from jax import lax
from jax.experimental import pallas as pl
from jax.experimental.pallas import tpu as pltpu
from jax.sharding import PartitionSpec as P

T = 512
B = 128
NB = 2 * T // B
RN = 32
RR = T // RN
CR = 64
L16 = 4 * T // B
SCHED = (8, 8, 8, 8)
HI = lax.Precision.HIGHEST
MESH = pl.DeviceIdType.MESH
F32 = jnp.float32
BF16 = jnp.bfloat16


def mm(a, b, dims=((1,), (0,)), precision=None):
    return lax.dot_general(a, b, (dims, ((), ())), precision=precision, preferred_element_type=F32)


def split(x):
    h = x.astype(BF16)
    return h, (x - h.astype(F32)).astype(BF16)


def mm3(a, b, dims=((1,), (0,))):
    return mm(a[0], b[0], dims) + (mm(a[0], b[1], dims) + mm(a[1], b[0], dims))


def base(a, w):
    out = []
    sub = lax.broadcasted_iota(jnp.int32, (8, B), 0)
    lane = lambda x, k: jnp.broadcast_to(x[:, k : k + 1], (8, B))
    row = lambda x, m: jnp.broadcast_to(x[m : m + 1, :], (8, B))
    for g in range(16):
        cg = [lane(a[g], 8 * g + n) for n in range(8)]
        e = [[row(cg[n], m) if n >= m else None for n in range(8)] for m in range(8)]
        ar = [row(a[g], m) for m in range(8)]
        wr = [row(w[g], m) for m in range(8)]
        rs = [None] * 8
        u = [[None] * 8 for _ in range(8)]
        for m in range(8):
            rs[m] = lax.rsqrt(e[m][m])
            for n in range(m + 1, 8):
                u[m][n] = e[m][n] * rs[m]
            ar[m] = ar[m] * rs[m]
            wr[m] = wr[m] * rs[m]
            for m2 in range(m + 1, 8):
                for n in range(m2, 8):
                    e[m2][n] = e[m2][n] - u[m][m2] * u[m][n]
                ar[m2] = ar[m2] - u[m][m2] * ar[m]
                wr[m2] = wr[m2] - u[m][m2] * wr[m]
        o = wr[0]
        for m in range(1, 8):
            o = jnp.where(sub == m, wr[m], o)
        out.append(o)
        for h in range(g + 1, 16):
            c = [lane(a[h], 8 * g + n) for n in range(8)]
            for m in range(8):
                f = c[m] * rs[m]
                for n in range(m + 1, 8):
                    c[n] = c[n] - f * u[m][n]
                a[h] = a[h] - f * ar[m]
                w[h] = w[h] - f * wr[m]
    return out


def kernel(
    x, xq, abuf, rbuf, cbuf, fbuf, dbuf, vh, vl, lh, ll, wbuf, sbuf, part, vx, v_s, v_rec,
    r_rec, c_rec, f_rec, d_rec, rz_s, rx_s, rs_s, cy_s, cx_s, cs_s, f_s, d_s, loc,
):
    p, q, d = lax.axis_index("row"), lax.axis_index("col"), lax.axis_index("depth")
    z, xl = p // 2, p % 2
    y, xh = q // 2, q % 2
    xx = xh * 2 + xl
    dev = lambda zz, xli, yy, xhi, dd: (zz * 2 + xli, yy * 2 + xhi, dd)
    sib = dev(z, xl, y, xh, 1 - d)
    both = jnp.logical_and

    def remote(src, dst, ssem, rsem, to):
        return pltpu.make_async_remote_copy(
            src_ref=src, dst_ref=dst, send_sem=ssem, recv_sem=rsem, device_id=to, device_id_type=MESH
        )

    def arrived(dst, rsem):
        pltpu.make_async_copy(dst, dst, rsem).wait()

    def when_start(cond, copy, op):
        @pl.when(cond)
        def _():
            c = copy()
            c.start() if op else c.wait_send()

    is_root = both(both(p == 0, q == 0), d == 1)
    src_r = z == 0
    src_c = y == 0

    own = [
        pltpu.make_async_copy(
            x.at[pl.ds(pl.multiple_of((s * T + d * 256) * L16, 8), 256 * L16), :],
            abuf.at[pl.ds(s * 256 * L16, 256 * L16), :],
            loc.at[s],
        )
        for s in range(2)
    ]
    for c in own:
        c.start()
    r_loc = pltpu.make_async_copy(
        x.at[pl.ds(0, T * L16), :], rbuf.at[pl.ds(pl.multiple_of(xl * T * L16, 8), T * L16), :], loc.at[2]
    )
    c_loc = [
        pltpu.make_async_copy(
            xq.at[pl.ds(s * T + d * 256, 256), 0], cbuf.at[xh, pl.ds(d * T + s * 256, 256)], loc.at[3 + s]
        )
        for s in range(2)
    ]
    d_loc = pltpu.make_async_copy(xq.at[pl.ds(0, T), 0], dbuf.at[0, pl.ds(0, T)], loc.at[5])

    @pl.when(src_r)
    def _():
        r_loc.start()

    @pl.when(src_c)
    def _():
        for c in c_loc:
            c.start()

    @pl.when(is_root)
    def _():
        d_loc.start()

    near = [
        sib,
        dev((z + 1) % 8, xl, y, xh, d), dev((z + 7) % 8, xl, y, xh, d),
        dev(z, xl, (y + 1) % 4, xh, d), dev(z, xl, (y + 3) % 4, xh, d),
        dev(z, 1 - xl, y, xh, d), dev(z, xl, y, 1 - xh, d), dev(z, 1 - xl, y, 1 - xh, d),
    ]
    barrier = pltpu.get_barrier_semaphore()
    for to in near:
        pl.semaphore_signal(barrier, inc=1, device_id=to, device_id_type=MESH)
    pl.semaphore_wait(barrier, len(near))

    rpiece = lambda k, n: rbuf.at[pl.ds(pl.multiple_of((k * T + n * RR) * L16, 8), RR * L16), :]
    xr = lambda n: x.at[pl.ds(pl.multiple_of(n * RR * L16, 8), RR * L16), :]

    def cpiece(k, h, s, r):
        return cbuf.at[k, pl.ds(h * T + s * 256 + r * CR, CR)]

    xc = lambda h, s, r: xq.at[pl.ds(s * T + h * 256 + r * CR, CR), 0]
    fpiece = lambda b, c: fbuf.at[pl.ds(pl.multiple_of(b * B, B), B), pl.ds(pl.multiple_of(c * B, B), B)]

    def r_ring(n, src):
        nxt = jnp.where(n % 2 == 0, (z + 1) % 8, (z + 7) % 8)
        return remote(src, rpiece(xl, n), rz_s.at[n], r_rec.at[xl, n], dev(nxt, xl, y, xh, 0))

    def r_cross(n, src):
        return remote(src, rpiece(xl, n), rx_s.at[n], r_rec.at[xl, n], dev(z, 1 - xl, y, xh, 0))

    def r_sib(k, n, op):
        when_start(
            z >= 0, lambda: remote(rpiece(k, n), rpiece(k, n), rs_s.at[k, n], r_rec.at[k, n], sib), op
        )

    def c_next(k, h, s, r, src, more, op):
        i = (k * 2 + s) * 4 + r
        nxt = jnp.where(h == 0, (y + 1) % 4, (y + 3) % 4)
        when_start(
            more, lambda: remote(src, cpiece(k, h, s, r), cy_s.at[h, i], c_rec.at[h, i], dev(z, xl, nxt, xh, 0)), op
        )

    def c_cross(k, h, s, r, src, op):
        i = (k * 2 + s) * 4 + r
        when_start(
            y == (r + 2 * h) % 4,
            lambda: remote(src, cpiece(k, h, s, r), cx_s.at[h, i], c_rec.at[h, i], dev(z, xl, y, 1 - xh, 0)), op,
        )

    def c_sib(k, h, s, r, op):
        i = (k * 2 + s) * 4 + r
        when_start(
            h == 1,
            lambda: remote(cpiece(k, h, s, r), cpiece(k, h, s, r), cs_s.at[i], c_rec.at[h, i], sib), op,
        )

    def f_send(b, c, op):
        v = fpiece(b, c)
        i = b * NB + c
        go = lambda cond, slot, to: when_start(
            cond, lambda: remote(v, v, f_s.at[slot, i], f_rec.at[i], to), op
        )
        root_line = both(z == 0, y == 0)
        go(both(root_line, xx == 0), 0, dev(z, 1, y, 0, 1))
        go(both(root_line, xx == 0), 1, dev(z, 1, y, 1, 1))
        go(both(root_line, xx == 1), 1, dev(z, 0, y, 1, 1))
        plane = y == 0
        go(both(plane, z <= 3), 2, dev((z + 1) % 8, xl, y, xh, 1))
        go(both(plane, (z == 0) | (z >= 6)), 3, dev((z + 7) % 8, xl, y, xh, 1))
        go((y == 0) | (y == 1), 4, dev(z, xl, (y + 1) % 4, xh, 1))
        go(y == 0, 5, dev(z, xl, (y + 3) % 4, xh, 1))
        go(z >= 0, 6, sib)

    def loop(n, f):
        lax.fori_loop(0, n, lambda i, s: (f(i), s)[1], 0)

    def d_copies(op):
        for i in range(4):
            when_start(
                both(both(p == 0, q == 1), d == 1),
                lambda: remote(
                    xq.at[pl.ds(i * B, B), 0], dbuf.at[1, pl.ds(i * B, B)], d_s.at[i], d_rec.at[i], (0, 0, 1)
                ),
                op,
            )
        when_start(
            both(both(p == 1, q == 1), d == 1),
            lambda: remote(
                xq.at[pl.ds(0, T), 0], dbuf.at[1, pl.ds(T, T)], d_s.at[4], d_rec.at[4], (0, 0, 1)
            ),
            op,
        )

    d_copies(True)

    def source_copies(op):
        @pl.when(both(src_c, d == 0))
        def _():
            def one(i):
                s, r = i // 4, i % 4
                for h in range(2):
                    c_next(xh, h, s, r, xc(h, s, r), z >= 0, op)
                    c_cross(xh, h, s, r, xc(h, s, r), op)

            loop(8, one)

    def forward(op):
        def own_line(t):
            if op:
                @pl.when(z == 0)
                def _():
                    @pl.when(t < RN // 2)
                    def _():
                        for up in range(2):
                            r_ring(2 * t + up, xr(2 * t + up)).start()

                    @pl.when(t < RN)
                    def _():
                        r_cross(t, xr(t)).start()

                    o = t - 3

                    @pl.when(both(o >= 0, o < RN // 2))
                    def _():
                        for up in range(2):
                            r_ring(2 * o + up, xr(2 * o + up)).wait_send()

                    @pl.when(both(o >= 0, o < RN))
                    def _():
                        r_cross(o, xr(o)).wait_send()

            for up in range(2):
                hops = z if up == 0 else 8 - z
                last = (z == 7) if up == 0 else (z == 1)
                first = 3 * hops
                e = t - first
                n = 2 * e + up

                @pl.when(both(both(e >= 0, e < RN // 2), z != 0))
                def _():
                    if op:
                        arrived(rpiece(xl, n), r_rec.at[xl, n])
                    when_start(jnp.logical_not(last), lambda: r_ring(n, rpiece(xl, n)), op)
                    when_start(z >= 0, lambda: r_cross(n, rpiece(xl, n)), op)
                    r_sib(xl, n, op)

            for h in range(2):
                hops = y if h == 0 else (4 - y) % 4
                e = t - 3 * hops
                on = z >= 0

                @pl.when(both(both(e >= 0, e < 8), both(y != 0, on)))
                def _():
                    s, r = e // 4, e % 4
                    if op:
                        arrived(cpiece(xh, h, s, r), c_rec.at[h, (xh * 2 + s) * 4 + r])
                    c_next(xh, h, s, r, cpiece(xh, h, s, r), hops != 3, op)
                    c_cross(xh, h, s, r, cpiece(xh, h, s, r), op)
                    c_sib(xh, h, s, r, op)

        def other_line(j):
            for h in range(2):
                r = (y + j + 2 * h) % 4 if h else (y - j + 4) % 4
                for s in range(2):
                    k = 1 - xh
                    if op:
                        arrived(cpiece(k, h, s, r), c_rec.at[h, (k * 2 + s) * 4 + r])
                    c_next(k, h, s, r, cpiece(k, h, s, r), j != 3, op)
                    c_sib(k, h, s, r, op)

        def step(t):
            own_line(t)
            for j in range(4):

                @pl.when(t == 20 + 4 * j)
                def _():
                    other_line(j)

        loop(5 + RN, step)

    def across(half, op):
        def one(i):
            n = half * (RN // 2) + i
            if op:
                arrived(rpiece(1 - xl, n), r_rec.at[1 - xl, n])
            r_sib(1 - xl, n, op)

        loop(RN // 2, one)

    source_copies(True)

    @pl.when(is_root)
    def _():
        d_loc.wait()
        lanes = lax.broadcasted_iota(jnp.int32, (8, B), 1)
        subs = lax.broadcasted_iota(jnp.int32, (8, B), 0)

        def dblock(v, c):
            return dbuf[c // 4, v * B : (v + 1) * B, c % 4, :]

        def factor(b):
            for v in range(NB):

                @pl.when(b == v)
                def _():
                    if v == 4:
                        arrived(dbuf.at[1, pl.ds(T, T)], d_rec.at[4])
                    s = dblock(v, v)
                    if v:
                        u = fbuf[: v * B, v * B : (v + 1) * B]
                        s = s - mm(u, u, ((0,), (0,)), HI)
                    sbuf[:, :B] = s

            a = [sbuf[8 * h : 8 * h + 8, 0:B] for h in range(16)]
            w = [jnp.where(lanes == subs + 8 * h, 1.0, 0.0) for h in range(16)]
            o = base(a, w)
            for v in range(NB):

                @pl.when(b == v)
                def _():
                    for h in range(16):
                        fbuf[v * B + 8 * h : v * B + 8 * h + 8, v * B : (v + 1) * B] = o[h]
                    if v < 4:
                        arrived(dbuf.at[1, pl.ds(v * B, B)], d_rec.at[v])
                    if v < NB - 1:
                        s = jnp.concatenate([dblock(v, c) for c in range(v + 1, NB)], axis=1)
                        if v:
                            s = s - mm(
                                fbuf[: v * B, v * B : (v + 1) * B], fbuf[: v * B, (v + 1) * B :], ((0,), (0,)), HI
                            )
                        wv = fbuf[v * B : (v + 1) * B, v * B : (v + 1) * B]
                        fbuf[v * B : (v + 1) * B, (v + 1) * B :] = mm(wv, s, precision=HI)

            lax.fori_loop(b, NB, lambda c, s: (f_send(b, c, True), s)[1], 0)

        loop(NB, factor)

    @pl.when(d == 0)
    def _():
        forward(True)

    passes = both(d == 1, jnp.logical_not(is_root))

    def pass_on(b, c):
        arrived(fpiece(b, c), f_rec.at[b * NB + c])
        f_send(b, c, True)

    def take(b, c):
        arrived(fpiece(b, c), f_rec.at[b * NB + c])

    def f_rows(first, last, f):
        def rows(b, _):
            lax.fori_loop(b, NB, lambda c, s: (f(b, c), s)[1], 0)
            return 0

        lax.fori_loop(first, last, rows, 0)

    def panels_here(k, half):
        @pl.when(d == 1)
        def _():
            def one(i):
                n = half * (RN // 2) + i

                @pl.when((z != 0) | (k != xl))
                def _():
                    arrived(rpiece(k, n), r_rec.at[k, n])

            loop(RN // 2, one)

            def two(i):
                @pl.when((y != 0) | (k != xh))
                def _():
                    arrived(cpiece(k, 1, i // 4, i % 4), c_rec.at[1, k * 8 + i])

            if half == 0:
                loop(8, two)

        if half == 0:

            @pl.when(both(src_r, k == xl))
            def _():
                r_loc.wait()

            @pl.when(both(src_c, k == xh))
            def _():
                for c in c_loc:
                    c.wait()

    G = 256
    crow = pl.ds(d * T, T)

    def rload(at, n):
        return jnp.concatenate([rbuf[pl.ds(at * L16 + n * 4 + c, G, stride=L16), :] for c in range(4)], axis=1)

    def v_copy(g, i):
        n = 2 * d + i
        v = vx.at[pl.ds(g * G, G), pl.ds(pl.multiple_of(n * T, B), T)]
        return remote(v, v, v_s.at[g * 2 + i], v_rec.at[g * 4 + n], sib)

    def aload(s, n):
        return jnp.concatenate(
            [abuf[pl.ds(s * 256 * L16 + n * 4 + c, 256, stride=L16), :] for c in range(4)], axis=1
        )

    def astore(s, n, val):
        for c in range(4):
            abuf[pl.ds(s * 256 * L16 + n * 4 + c, 256, stride=L16), :] = val[:, c * B : (c + 1) * B]

    for g in range(2 * T // G):
        at = g * G
        if SCHED[g] > (SCHED[g - 1] if g else 0):

            @pl.when(passes)
            def _():
                f_rows(SCHED[g - 1] if g else 0, SCHED[g], pass_on)

        if g < 2:

            @pl.when(d == 0)
            def _():
                across(g, True)

        panels_here(g // 2, g % 2)
        if g == 0:
            for c in own:
                c.wait()
        c4 = (at % T) // B
        acc = jnp.concatenate([cbuf[g // 2, crow, c4 + c, :] for c in range(2)], axis=1)
        if g:
            uf = fbuf[:at, at : at + G]
            u = split(uf)
            ut = split(uf.T)
            acc = acc - mm3((lh[:, :at], ll[:, :at]), u)

            def before(i):
                n = 2 * d + i
                cols = pl.ds(pl.multiple_of(n * T, B), T)
                part[:, cols] = rload(at, n) - mm3(ut, (vh[:at, cols], vl[:at, cols]))

            loop(2, before)
        wbuf[:, :G] = acc

        @pl.when(d == 0)
        def _():
            f_rows(2 * g, 2 * g + 2, take)

        w1 = fbuf[at : at + B, at : at + B]
        w2 = fbuf[at + B : at + G, at + B : at + G]
        u12 = fbuf[at : at + B, at + B : at + G]
        w21 = -mm(w2, mm(u12, w1, ((0,), (0,)), HI), precision=HI)
        w = jnp.concatenate(
            [jnp.concatenate([w1, jnp.zeros((B, B), F32)], axis=1), jnp.concatenate([w21, w2], axis=1)], axis=0
        )
        wt = split(w.T)
        w = split(w)

        def solve(i):
            n = 2 * d + i
            cols = pl.ds(pl.multiple_of(n * T, B), T)
            v = mm3(w, split(part[:, cols] if g else rload(at, n)))
            vx[at : at + G, cols] = v
            a, b = split(v)
            vh[at : at + G, cols] = a
            vl[at : at + G, cols] = b
            v_copy(g, i).start()

        loop(2, solve)
        la, lb = split(mm3(split(wbuf[...]), wt))
        lh[:, at : at + G] = la
        ll[:, at : at + G] = lb

    def there(i):
        rows = pl.ds(pl.multiple_of((i // 2) * G, G), G)
        n = 2 * (1 - d) + i % 2
        cols = pl.ds(pl.multiple_of(n * T, B), T)
        arrived(vx.at[rows, cols], v_rec.at[(i // 2) * 4 + n])
        a, b = split(vx[rows, cols])
        vh[rows, cols] = a
        vl[rows, cols] = b

    loop(8, there)

    def update(n):
        cols = pl.ds(pl.multiple_of(n * T, B), T)
        for s in range(2):
            rows = slice(s * 256, s * 256 + 256)
            res = aload(s, n) - mm3((lh[rows, :], ll[rows, :]), (vh[:, cols], vl[:, cols]))
            if s == 0:
                res = jnp.where(p < 2, 0.0, res)
            astore(s, n, res)

    loop(4, update)

    @pl.when(q < 2)
    def _():
        pick = pl.ds(pl.multiple_of(q * T, B), T)
        for s in range(2):
            rows = slice(s * 256, s * 256 + 256)
            res = lh[rows, pick].astype(F32) + ll[rows, pick].astype(F32)
            if s == 0:
                i = lax.broadcasted_iota(jnp.int32, (256, T), 0) + d * 256
                j = lax.broadcasted_iota(jnp.int32, (256, T), 1)
                res = jnp.where((p > q) | ((p == q) & (i >= j)), res, 0.0)
            astore(s, 0, res)

    for g in range(4):
        loop(2, lambda i: v_copy(g, i).wait_send())
    d_copies(False)
    source_copies(False)

    @pl.when(d == 0)
    def _():
        forward(False)
        across(0, False)
        across(1, False)

    @pl.when(d == 1)
    def _():
        f_rows(0, NB, lambda b, c: f_send(b, c, False))


def call(x, xq):
    dma = pltpu.SemaphoreType.DMA
    return pl.pallas_call(
        kernel,
        out_shape=pltpu.VMEM((T * L16, B), F32),
        in_specs=[pl.BlockSpec(memory_space=pltpu.HBM)] * 2,
        out_specs=pl.BlockSpec(memory_space=pltpu.VMEM),
        scratch_shapes=[
            pltpu.VMEM((2 * T * L16, B), F32),
            pltpu.VMEM((2, 2 * T, 4, B), F32),
            pltpu.VMEM((2 * T, 2 * T), F32),
            pltpu.VMEM((2, 2 * T, 4, B), F32),
            pltpu.VMEM((2 * T, 4 * T), BF16),
            pltpu.VMEM((2 * T, 4 * T), BF16),
            pltpu.VMEM((T, 2 * T), BF16),
            pltpu.VMEM((T, 2 * T), BF16),
            pltpu.VMEM((T, 256), F32),
            pltpu.VMEM((B, B), F32),
            pltpu.VMEM((256, 4 * T), F32),
            pltpu.VMEM((2 * T, 4 * T), F32),
            dma((8,)),
            dma((16,)),
            dma((2, RN)),
            dma((2, 16)),
            dma((NB * NB,)),
            dma((5,)),
            dma((RN,)),
            dma((RN,)),
            dma((2, RN)),
            dma((2, 16)),
            dma((2, 16)),
            dma((16,)),
            dma((7, NB * NB)),
            dma((5,)),
            dma((7,)),
        ],
        compiler_params=pltpu.CompilerParams(collective_id=0, has_side_effects=True, vmem_limit_bytes=56 * 1024 * 1024),
        name="panels",
    )(x, xq)


def body(matrix):
    out = call(matrix.reshape(2 * T * L16, B), matrix.reshape(2 * T, 4, 4, B))
    return out.reshape(2, 1, T // 2, 4, 1, T)


def solution(mesh):
    return jax.shard_map(
        body,
        mesh=mesh,
        in_specs=(P(None, "row", None, None, "col", None),),
        out_specs=P(None, "row", "depth", None, "col", None),
        check_vma=False,
    )
```

```python
import functools

import jax
import jax.numpy as jnp
from jax import lax
from jax.experimental import pallas as pl
from jax.experimental.pallas import tpu as pltpu
from jax.sharding import PartitionSpec as P

T = 512
B = 128
NB = 2 * T // B
RN = 32
RR = T // RN
CR = 64
L16 = 4 * T // B
SCHED = (8, 8, 8, 8)
HI = lax.Precision.HIGHEST
MESH = pl.DeviceIdType.MESH
F32 = jnp.float32
BF16 = jnp.bfloat16


def mm(a, b, dims=((1,), (0,)), precision=None):
    return lax.dot_general(a, b, (dims, ((), ())), precision=precision, preferred_element_type=F32)


def split(x):
    h = x.astype(BF16)
    return h, (x - h.astype(F32)).astype(BF16)


def mm3(a, b, dims=((1,), (0,))):
    return mm(a[0], b[0], dims) + (mm(a[0], b[1], dims) + mm(a[1], b[0], dims))


def base(a, w):
    out = []
    sub = lax.broadcasted_iota(jnp.int32, (8, B), 0)
    lane = lambda x, k: jnp.broadcast_to(x[:, k : k + 1], (8, B))
    row = lambda x, m: jnp.broadcast_to(x[m : m + 1, :], (8, B))
    for g in range(16):
        cg = [lane(a[g], 8 * g + n) for n in range(8)]
        e = [[row(cg[n], m) if n >= m else None for n in range(8)] for m in range(8)]
        ar = [row(a[g], m) for m in range(8)]
        wr = [row(w[g], m) for m in range(8)]
        rs = [None] * 8
        u = [[None] * 8 for _ in range(8)]
        for m in range(8):
            rs[m] = lax.rsqrt(e[m][m])
            for n in range(m + 1, 8):
                u[m][n] = e[m][n] * rs[m]
            ar[m] = ar[m] * rs[m]
            wr[m] = wr[m] * rs[m]
            for m2 in range(m + 1, 8):
                for n in range(m2, 8):
                    e[m2][n] = e[m2][n] - u[m][m2] * u[m][n]
                ar[m2] = ar[m2] - u[m][m2] * ar[m]
                wr[m2] = wr[m2] - u[m][m2] * wr[m]
        o = wr[0]
        for m in range(1, 8):
            o = jnp.where(sub == m, wr[m], o)
        out.append(o)
        for h in range(g + 1, 16):
            c = [lane(a[h], 8 * g + n) for n in range(8)]
            for m in range(8):
                f = c[m] * rs[m]
                for n in range(m + 1, 8):
                    c[n] = c[n] - f * u[m][n]
                a[h] = a[h] - f * ar[m]
                w[h] = w[h] - f * wr[m]
    return out


def kernel(
    x, xq, abuf, rbuf, cbuf, fbuf, dbuf, vh, vl, lh, ll, wbuf, sbuf, part, vx, v_s, v_rec,
    r_rec, c_rec, f_rec, d_rec, rz_s, rx_s, rs_s, cy_s, cx_s, cs_s, f_s, d_s, loc,
):
    p, q, d = lax.axis_index("row"), lax.axis_index("col"), lax.axis_index("depth")
    z, xl = p // 2, p % 2
    y, xh = q // 2, q % 2
    xx = xh * 2 + xl
    dev = lambda zz, xli, yy, xhi, dd: (zz * 2 + xli, yy * 2 + xhi, dd)
    sib = dev(z, xl, y, xh, 1 - d)
    both = jnp.logical_and

    def remote(src, dst, ssem, rsem, to):
        return pltpu.make_async_remote_copy(
            src_ref=src, dst_ref=dst, send_sem=ssem, recv_sem=rsem, device_id=to, device_id_type=MESH
        )

    def arrived(dst, rsem):
        pltpu.make_async_copy(dst, dst, rsem).wait()

    def when_start(cond, copy, op):
        @pl.when(cond)
        def _():
            c = copy()
            c.start() if op else c.wait_send()

    is_root = both(both(p == 0, q == 0), d == 1)
    src_r = z == 0
    src_c = y == 0

    own = [
        pltpu.make_async_copy(
            x.at[pl.ds(pl.multiple_of((s * T + d * 256) * L16, 8), 256 * L16), :],
            abuf.at[pl.ds(s * 256 * L16, 256 * L16), :],
            loc.at[s],
        )
        for s in range(2)
    ]
    for c in own:
        c.start()
    r_loc = pltpu.make_async_copy(
        x.at[pl.ds(0, T * L16), :], rbuf.at[pl.ds(pl.multiple_of(xl * T * L16, 8), T * L16), :], loc.at[2]
    )
    c_loc = [
        pltpu.make_async_copy(
            xq.at[pl.ds(s * T + d * 256, 256), 0], cbuf.at[xh, pl.ds(d * T + s * 256, 256)], loc.at[3 + s]
        )
        for s in range(2)
    ]
    d_loc = pltpu.make_async_copy(xq.at[pl.ds(0, T), 0], dbuf.at[0, pl.ds(0, T)], loc.at[5])

    @pl.when(src_r)
    def _():
        r_loc.start()

    @pl.when(src_c)
    def _():
        for c in c_loc:
            c.start()

    @pl.when(is_root)
    def _():
        d_loc.start()

    near = [
        sib,
        dev((z + 1) % 8, xl, y, xh, d), dev((z + 7) % 8, xl, y, xh, d),
        dev(z, xl, (y + 1) % 4, xh, d), dev(z, xl, (y + 3) % 4, xh, d),
        dev(z, 1 - xl, y, xh, d), dev(z, xl, y, 1 - xh, d), dev(z, 1 - xl, y, 1 - xh, d),
    ]
    barrier = pltpu.get_barrier_semaphore()
    for to in near:
        pl.semaphore_signal(barrier, inc=1, device_id=to, device_id_type=MESH)
    pl.semaphore_wait(barrier, len(near))

    rpiece = lambda k, n: rbuf.at[pl.ds(pl.multiple_of((k * T + n * RR) * L16, 8), RR * L16), :]
    xr = lambda n: x.at[pl.ds(pl.multiple_of(n * RR * L16, 8), RR * L16), :]

    def cpiece(k, h, s, r):
        return cbuf.at[k, pl.ds(h * T + s * 256 + r * CR, CR)]

    xc = lambda h, s, r: xq.at[pl.ds(s * T + h * 256 + r * CR, CR), 0]
    fpiece = lambda b, c: fbuf.at[pl.ds(pl.multiple_of(b * B, B), B), pl.ds(pl.multiple_of(c * B, B), B)]

    def r_ring(n, src):
        nxt = jnp.where(n % 2 == 0, (z + 1) % 8, (z + 7) % 8)
        return remote(src, rpiece(xl, n), rz_s.at[n], r_rec.at[xl, n], dev(nxt, xl, y, xh, 0))

    def r_cross(n, src):
        return remote(src, rpiece(xl, n), rx_s.at[n], r_rec.at[xl, n], dev(z, 1 - xl, y, xh, 0))

    def r_sib(k, n, op):
        when_start(
            z >= 0, lambda: remote(rpiece(k, n), rpiece(k, n), rs_s.at[k, n], r_rec.at[k, n], sib), op
        )

    def c_next(k, h, s, r, src, more, op):
        i = (k * 2 + s) * 4 + r
        nxt = jnp.where(h == 0, (y + 1) % 4, (y + 3) % 4)
        when_start(
            more, lambda: remote(src, cpiece(k, h, s, r), cy_s.at[h, i], c_rec.at[h, i], dev(z, xl, nxt, xh, 0)), op
        )

    def c_cross(k, h, s, r, src, op):
        i = (k * 2 + s) * 4 + r
        when_start(
            y == (r + 2 * h) % 4,
            lambda: remote(src, cpiece(k, h, s, r), cx_s.at[h, i], c_rec.at[h, i], dev(z, xl, y, 1 - xh, 0)), op,
        )

    def c_sib(k, h, s, r, op):
        i = (k * 2 + s) * 4 + r
        when_start(
            h == 1,
            lambda: remote(cpiece(k, h, s, r), cpiece(k, h, s, r), cs_s.at[i], c_rec.at[h, i], sib), op,
        )

    def f_send(b, c, op):
        v = fpiece(b, c)
        i = b * NB + c
        go = lambda cond, slot, to: when_start(
            cond, lambda: remote(v, v, f_s.at[slot, i], f_rec.at[i], to), op
        )
        root_line = both(z == 0, y == 0)
        go(both(root_line, xx == 0), 0, dev(z, 1, y, 0, 1))
        go(both(root_line, xx == 0), 1, dev(z, 1, y, 1, 1))
        go(both(root_line, xx == 1), 1, dev(z, 0, y, 1, 1))
        plane = y == 0
        go(both(plane, z <= 3), 2, dev((z + 1) % 8, xl, y, xh, 1))
        go(both(plane, (z == 0) | (z >= 6)), 3, dev((z + 7) % 8, xl, y, xh, 1))
        go((y == 0) | (y == 1), 4, dev(z, xl, (y + 1) % 4, xh, 1))
        go(y == 0, 5, dev(z, xl, (y + 3) % 4, xh, 1))
        go(z >= 0, 6, sib)

    def loop(n, f):
        lax.fori_loop(0, n, lambda i, s: (f(i), s)[1], 0)

    def d_copies(op):
        for i in range(4):
            when_start(
                both(both(p == 0, q == 1), d == 1),
                lambda: remote(
                    xq.at[pl.ds(i * B, B), 0], dbuf.at[1, pl.ds(i * B, B)], d_s.at[i], d_rec.at[i], (0, 0, 1)
                ),
                op,
            )
        when_start(
            both(both(p == 1, q == 1), d == 1),
            lambda: remote(
                xq.at[pl.ds(0, T), 0], dbuf.at[1, pl.ds(T, T)], d_s.at[4], d_rec.at[4], (0, 0, 1)
            ),
            op,
        )

    d_copies(True)

    def c_source(i, op):
        @pl.when(both(src_c, d == 0))
        def _():
            s, r = i // 4, i % 4
            for h in range(2):
                c_next(xh, h, s, r, xc(h, s, r), z >= 0, op)
                c_cross(xh, h, s, r, xc(h, s, r), op)

    def forward(op):
        def own_line(t):
            if op:
                @pl.when(z == 0)
                def _():
                    @pl.when(t < RN // 2)
                    def _():
                        for up in range(2):
                            r_ring(2 * t + up, xr(2 * t + up)).start()

                    @pl.when(t < RN)
                    def _():
                        r_cross(t, xr(t)).start()

                    o = t - 4

                    @pl.when(both(o >= 0, o < RN // 2))
                    def _():
                        for up in range(2):
                            r_ring(2 * o + up, xr(2 * o + up)).wait_send()

                    i = t - 8

                    @pl.when(both(i >= 0, i < RN))
                    def _():
                        r_cross(i, xr(i)).wait_send()

            for up in range(2):
                hops = z if up == 0 else 8 - z
                last = (z == 7) if up == 0 else (z == 1)
                first = 3 * hops
                e = t - first
                n = 2 * e + up

                @pl.when(both(both(e >= 0, e < RN // 2), z != 0))
                def _():
                    if op:
                        arrived(rpiece(xl, n), r_rec.at[xl, n])
                    when_start(jnp.logical_not(last), lambda: r_ring(n, rpiece(xl, n)), op)
                    when_start(z >= 0, lambda: r_cross(n, rpiece(xl, n)), op)
                    r_sib(xl, n, op)

            for h in range(2):
                hops = y if h == 0 else (4 - y) % 4
                e = t - 3 * hops
                on = z >= 0

                @pl.when(both(both(e >= 0, e < 8), both(y != 0, on)))
                def _():
                    s, r = e // 4, e % 4
                    if op:
                        arrived(cpiece(xh, h, s, r), c_rec.at[h, (xh * 2 + s) * 4 + r])
                    c_next(xh, h, s, r, cpiece(xh, h, s, r), hops != 3, op)
                    c_cross(xh, h, s, r, cpiece(xh, h, s, r), op)
                    c_sib(xh, h, s, r, op)

        def other_line(j):
            for h in range(2):
                r = (y + j + 2 * h) % 4 if h else (y - j + 4) % 4
                for s in range(2):
                    k = 1 - xh
                    if op:
                        arrived(cpiece(k, h, s, r), c_rec.at[h, (k * 2 + s) * 4 + r])
                    c_next(k, h, s, r, cpiece(k, h, s, r), j != 3, op)
                    c_sib(k, h, s, r, op)

        def step(t):
            own_line(t)
            if op:

                @pl.when(t < 8)
                def _():
                    c_source(t, True)

            for j in range(4):

                @pl.when(t == 20 + 4 * j)
                def _():
                    other_line(j)

        loop(max(5, 8) + RN, step)

    def across(half, op):
        def one(i):
            n = half * (RN // 2) + i
            if op:
                arrived(rpiece(1 - xl, n), r_rec.at[1 - xl, n])
            r_sib(1 - xl, n, op)

        loop(RN // 2, one)

    @pl.when(is_root)
    def _():
        d_loc.wait()
        lanes = lax.broadcasted_iota(jnp.int32, (8, B), 1)
        subs = lax.broadcasted_iota(jnp.int32, (8, B), 0)

        def dblock(v, c):
            return dbuf[c // 4, v * B : (v + 1) * B, c % 4, :]

        def factor(b):
            for v in range(NB):

                @pl.when(b == v)
                def _():
                    if v == 4:
                        arrived(dbuf.at[1, pl.ds(T, T)], d_rec.at[4])
                    s = dblock(v, v)
                    if v:
                        u = fbuf[: v * B, v * B : (v + 1) * B]
                        s = s - mm(u, u, ((0,), (0,)), HI)
                    sbuf[:, :B] = s

            a = [sbuf[8 * h : 8 * h + 8, 0:B] for h in range(16)]
            w = [jnp.where(lanes == subs + 8 * h, 1.0, 0.0) for h in range(16)]
            o = base(a, w)
            for v in range(NB):

                @pl.when(b == v)
                def _():
                    for h in range(16):
                        fbuf[v * B + 8 * h : v * B + 8 * h + 8, v * B : (v + 1) * B] = o[h]
                    if v < 4:
                        arrived(dbuf.at[1, pl.ds(v * B, B)], d_rec.at[v])
                    if v < NB - 1:
                        s = jnp.concatenate([dblock(v, c) for c in range(v + 1, NB)], axis=1)
                        if v:
                            s = s - mm(
                                fbuf[: v * B, v * B : (v + 1) * B], fbuf[: v * B, (v + 1) * B :], ((0,), (0,)), HI
                            )
                        wv = fbuf[v * B : (v + 1) * B, v * B : (v + 1) * B]
                        fbuf[v * B : (v + 1) * B, (v + 1) * B :] = mm(wv, s, precision=HI)

            lax.fori_loop(b, NB, lambda c, s: (f_send(b, c, True), s)[1], 0)

        loop(NB, factor)

    @pl.when(d == 0)
    def _():
        forward(True)

    passes = both(d == 1, jnp.logical_not(is_root))

    def pass_on(b, c):
        arrived(fpiece(b, c), f_rec.at[b * NB + c])
        f_send(b, c, True)

    def take(b, c):
        arrived(fpiece(b, c), f_rec.at[b * NB + c])

    def f_rows(first, last, f):
        def rows(b, _):
            lax.fori_loop(b, NB, lambda c, s: (f(b, c), s)[1], 0)
            return 0

        lax.fori_loop(first, last, rows, 0)

    def panels_here(k, half):
        @pl.when(d == 1)
        def _():
            def one(i):
                n = half * (RN // 2) + i

                @pl.when((z != 0) | (k != xl))
                def _():
                    arrived(rpiece(k, n), r_rec.at[k, n])

            loop(RN // 2, one)

            def two(i):
                @pl.when((y != 0) | (k != xh))
                def _():
                    arrived(cpiece(k, 1, i // 4, i % 4), c_rec.at[1, k * 8 + i])

            if half == 0:
                loop(8, two)

        if half == 0:

            @pl.when(both(src_r, k == xl))
            def _():
                r_loc.wait()

            @pl.when(both(src_c, k == xh))
            def _():
                for c in c_loc:
                    c.wait()

    G = 256
    crow = pl.ds(d * T, T)

    def rload(at, n):
        return jnp.concatenate([rbuf[pl.ds(at * L16 + n * 4 + c, G, stride=L16), :] for c in range(4)], axis=1)

    def v_copy(g, i):
        n = 2 * d + i
        v = vx.at[pl.ds(g * G, G), pl.ds(pl.multiple_of(n * T, B), T)]
        return remote(v, v, v_s.at[g * 2 + i], v_rec.at[g * 4 + n], sib)

    def aload(s, n):
        return jnp.concatenate(
            [abuf[pl.ds(s * 256 * L16 + n * 4 + c, 256, stride=L16), :] for c in range(4)], axis=1
        )

    def astore(s, n, val):
        for c in range(4):
            abuf[pl.ds(s * 256 * L16 + n * 4 + c, 256, stride=L16), :] = val[:, c * B : (c + 1) * B]

    for g in range(2 * T // G):
        at = g * G
        if SCHED[g] > (SCHED[g - 1] if g else 0):

            @pl.when(passes)
            def _():
                f_rows(SCHED[g - 1] if g else 0, SCHED[g], pass_on)

        @pl.when(both(d == 0, xl == (1 if g < 2 else 0)))
        def _():
            across(g % 2, True)

        panels_here(g // 2, g % 2)
        if g == 0:
            for c in own:
                c.wait()
        c4 = (at % T) // B
        acc = jnp.concatenate([cbuf[g // 2, crow, c4 + c, :] for c in range(2)], axis=1)
        if g:
            uf = fbuf[:at, at : at + G]
            u = split(uf)
            ut = split(uf.T)
            acc = acc - mm3((lh[:, :at], ll[:, :at]), u)

            def before(i):
                n = 2 * d + i
                cols = pl.ds(pl.multiple_of(n * T, B), T)
                part[:, cols] = rload(at, n) - mm3(ut, (vh[:at, cols], vl[:at, cols]))

            loop(2, before)
        wbuf[:, :G] = acc

        @pl.when(d == 0)
        def _():
            f_rows(2 * g, 2 * g + 2, take)

        w1 = fbuf[at : at + B, at : at + B]
        w2 = fbuf[at + B : at + G, at + B : at + G]
        u12 = fbuf[at : at + B, at + B : at + G]
        w21 = -mm(w2, mm(u12, w1, ((0,), (0,)), HI), precision=HI)
        w = jnp.concatenate(
            [jnp.concatenate([w1, jnp.zeros((B, B), F32)], axis=1), jnp.concatenate([w21, w2], axis=1)], axis=0
        )
        wt = split(w.T)
        w = split(w)

        def solve(i):
            n = 2 * d + i
            cols = pl.ds(pl.multiple_of(n * T, B), T)
            v = mm3(w, split(part[:, cols] if g else rload(at, n)))
            vx[at : at + G, cols] = v
            a, b = split(v)
            vh[at : at + G, cols] = a
            vl[at : at + G, cols] = b
            v_copy(g, i).start()

        loop(2, solve)
        la, lb = split(mm3(split(wbuf[...]), wt))
        lh[:, at : at + G] = la
        ll[:, at : at + G] = lb

    def there(i):
        rows = pl.ds(pl.multiple_of((i // 2) * G, G), G)
        n = 2 * (1 - d) + i % 2
        cols = pl.ds(pl.multiple_of(n * T, B), T)
        arrived(vx.at[rows, cols], v_rec.at[(i // 2) * 4 + n])
        a, b = split(vx[rows, cols])
        vh[rows, cols] = a
        vl[rows, cols] = b

    loop(8, there)

    def update(n):
        cols = pl.ds(pl.multiple_of(n * T, B), T)
        for s in range(2):
            rows = slice(s * 256, s * 256 + 256)
            res = aload(s, n) - mm3((lh[rows, :], ll[rows, :]), (vh[:, cols], vl[:, cols]))
            if s == 0:
                res = jnp.where(p < 2, 0.0, res)
            astore(s, n, res)

    loop(4, update)

    @pl.when(q < 2)
    def _():
        pick = pl.ds(pl.multiple_of(q * T, B), T)
        for s in range(2):
            rows = slice(s * 256, s * 256 + 256)
            res = lh[rows, pick].astype(F32) + ll[rows, pick].astype(F32)
            if s == 0:
                i = lax.broadcasted_iota(jnp.int32, (256, T), 0) + d * 256
                j = lax.broadcasted_iota(jnp.int32, (256, T), 1)
                res = jnp.where((p > q) | ((p == q) & (i >= j)), res, 0.0)
            astore(s, 0, res)

    for g in range(4):
        loop(2, lambda i: v_copy(g, i).wait_send())
    d_copies(False)
    loop(8, lambda i: c_source(i, False))

    @pl.when(d == 0)
    def _():
        forward(False)
        across(0, False)
        across(1, False)

    @pl.when(d == 1)
    def _():
        f_rows(0, NB, lambda b, c: f_send(b, c, False))


def call(x, xq):
    dma = pltpu.SemaphoreType.DMA
    return pl.pallas_call(
        kernel,
        out_shape=pltpu.VMEM((T * L16, B), F32),
        in_specs=[pl.BlockSpec(memory_space=pltpu.HBM)] * 2,
        out_specs=pl.BlockSpec(memory_space=pltpu.VMEM),
        scratch_shapes=[
            pltpu.VMEM((2 * T * L16, B), F32),
            pltpu.VMEM((2, 2 * T, 4, B), F32),
            pltpu.VMEM((2 * T, 2 * T), F32),
            pltpu.VMEM((2, 2 * T, 4, B), F32),
            pltpu.VMEM((2 * T, 4 * T), BF16),
            pltpu.VMEM((2 * T, 4 * T), BF16),
            pltpu.VMEM((T, 2 * T), BF16),
            pltpu.VMEM((T, 2 * T), BF16),
            pltpu.VMEM((T, 256), F32),
            pltpu.VMEM((B, B), F32),
            pltpu.VMEM((256, 4 * T), F32),
            pltpu.VMEM((2 * T, 4 * T), F32),
            dma((8,)),
            dma((16,)),
            dma((2, RN)),
            dma((2, 16)),
            dma((NB * NB,)),
            dma((5,)),
            dma((RN,)),
            dma((RN,)),
            dma((2, RN)),
            dma((2, 16)),
            dma((2, 16)),
            dma((16,)),
            dma((7, NB * NB)),
            dma((5,)),
            dma((7,)),
        ],
        compiler_params=pltpu.CompilerParams(collective_id=0, has_side_effects=True, vmem_limit_bytes=56 * 1024 * 1024),
        name="panels",
    )(x, xq)


def body(matrix):
    out = call(matrix.reshape(2 * T * L16, B), matrix.reshape(2 * T, 4, 4, B))
    return out.reshape(2, 1, T // 2, 4, 1, T)


def solution(mesh):
    return jax.shard_map(
        body,
        mesh=mesh,
        in_specs=(P(None, "row", None, None, "col", None),),
        out_specs=P(None, "row", "depth", None, "col", None),
        check_vma=False,
    )
```
